128 devices in a mesh: dp: 32 (over x, z, core), mp: 4 (over y).
Axes of the slice: x: 4, y: 4, z: 4, core: 2. Of those that a mesh axis runs over, the one named last changes fastest.
Arguments:
- partials: bfloat16 [32, 1024, 8192], P('dp', None, 'mp'), may hold values from -11 to 11
- momentum: float32 [128, 256, 256], P(('dp', 'mp')), may hold values from -0.3 to 0.3
- second: float32 [128, 256, 256], P(('dp', 'mp')), may hold values from 0.0002 to 0.02
- left_stat: float32 [128, 256, 256], P(('dp', 'mp')), may hold values from -36 to 36.5, as said below
- right_stat: float32 [128, 256, 256], P(('dp', 'mp')), may hold values from -36 to 36.5, as said below
- left_basis: float32 [128, 256, 256], P(('dp', 'mp')), may hold values from -1 to 1, as said below
- right_basis: float32 [128, 256, 256], P(('dp', 'mp')), may hold values from -1 to 1, as said below
Outputs:
- update: bfloat16 [1024, 8192], P(None, 'mp')
- momentum_new: float32 [128, 256, 256], P(('dp', 'mp'))
- second_new: float32 [128, 256, 256], P(('dp', 'mp'))
- left_new: float32 [128, 256, 256], P(('dp', 'mp'))
- right_new: float32 [128, 256, 256], P(('dp', 'mp'))
- left_basis_new: float32 [128, 256, 256], P(('dp', 'mp'))
- right_basis_new: float32 [128, 256, 256], P(('dp', 'mp'))
The draws below stay inside these ranges and needn't reach their ends.
Inputs may be any that keep to these rules, and one draw needn't show every extreme that they name: `left_stat`: each block is symmetric positive definite. `right_stat`: each block is symmetric positive definite. `left_basis`: each block is an orthogonal matrix. `right_basis`: each block is an orthogonal matrix.
All inputs are finite; a program needn't handle non-finite values.
Results may differ from the reference program's by a relative error of at most 0.00045.
Values may be sent and summed in bfloat16 or wider, within the bound.
A program may use at most 128 MiB of HBM per device.

```python
import math
import jax
import jax.numpy as jnp
from jax import lax

D = 8192
BLOCK = 256
TILES_DEV = 1
REPLICAS = 32
ROWS = 1024
TILES = 128
N_DP = 32
N_MP = 4


def draw_partials(key, part):
    keys = jax.random.split(jax.random.fold_in(key, 7), 4)
    row_scale = jnp.exp(jax.random.uniform(keys[0], (ROWS, 1), jnp.float32, 0.0, math.log(10.0)))
    col_scale = jnp.exp(jax.random.uniform(keys[1], (1, D), jnp.float32, 0.0, math.log(10.0)))
    position = jnp.arange(ROWS, dtype=jnp.float32)[:, None] / ROWS
    rise = 3.0 ** position
    noise = jnp.clip(jax.random.normal(keys[3], (REPLICAS, ROWS, D), jnp.float32), -6.0, 6.0)
    scale = 0.001 / math.sqrt(REPLICAS)
    return (scale * rise * row_scale * col_scale * noise).astype(jnp.bfloat16)


def spd_blocks(key):
    factor = jnp.clip(jax.random.normal(key, (TILES, BLOCK, BLOCK), jnp.float32), -6.0, 6.0)
    gram = jnp.einsum('tij,tkj->tik', factor, factor, precision=jax.lax.Precision.HIGHEST) / BLOCK
    return gram + 0.5 * jnp.eye(BLOCK, dtype=jnp.float32)[None]


def draw_left_stat(key, part):
    return spd_blocks(jax.random.fold_in(key, 11))


def draw_right_stat(key, part):
    return spd_blocks(jax.random.fold_in(key, 12))


def orthogonal_blocks(key):
    factor = jax.random.normal(key, (TILES, BLOCK, BLOCK), jnp.float32)
    basis, unused = jnp.linalg.qr(factor)
    return jnp.clip(basis, -1.0, 1.0)


def draw_left_basis(key, part):
    return orthogonal_blocks(jax.random.fold_in(key, 13))


def draw_right_basis(key, part):
    return orthogonal_blocks(jax.random.fold_in(key, 14))


def steps_of(own_key, extent, cuts, low, largest):
    gain = 1.0
    for axis_at, blocks in cuts:
        draws = jax.random.uniform(jax.random.fold_in(jax.random.fold_in(own_key, 6), axis_at), (blocks,), jnp.float32, low / len(cuts), largest / len(cuts))
        gain = gain * jnp.repeat(jnp.exp(draws), extent[axis_at] // blocks).reshape((-1,) + (1,) * (len(extent) - 1 - axis_at))
    return gain


def normal_values(own_key, extent, spread, limit, shards=(), held_as=jnp.bfloat16):
    level = steps_of(own_key, extent, shards, -0.22, 0.18) if shards else 1.0
    result = jax.random.normal(own_key, extent, jnp.float32) * spread * level
    return jnp.minimum(jnp.maximum(result, -limit), limit).astype(held_as)


def setup_inputs(seed: int = 0) -> dict:
    arg_keys = jax.random.split(jax.random.key(seed), 8)
    partials = draw_partials(jax.random.fold_in(arg_keys[7], 71), 0)
    momentum = normal_values(arg_keys[1], (TILES, BLOCK, BLOCK), 0.05, 0.3, ((0, 128),), jnp.float32)
    second = jnp.clip(jnp.exp(math.log(0.02) - 4.6051702 * jax.random.uniform(arg_keys[2], (TILES, BLOCK, BLOCK), jnp.float32) ** steps_of(arg_keys[2], (TILES, BLOCK, BLOCK), ((0, 128),), -0.2, 0.2)), 0.0002, 0.02)
    left_stat = draw_left_stat(jax.random.fold_in(arg_keys[7], 71), 0)
    right_stat = draw_right_stat(jax.random.fold_in(arg_keys[7], 71), 0)
    left_basis = draw_left_basis(jax.random.fold_in(arg_keys[7], 71), 0)
    right_basis = draw_right_basis(jax.random.fold_in(arg_keys[7], 71), 0)
    return {"partials": partials, "momentum": momentum, "second": second, "left_stat": left_stat, "right_stat": right_stat, "left_basis": left_basis, "right_basis": right_basis}


beta_first = 0.9
beta_second = 0.95
epsilon = 1e-08
highest = lax.Precision.HIGHEST

def product(left, right):
    return jnp.einsum('tij,tjk->tik', left, right, precision=highest)

def inner_left(left, right):
    return jnp.einsum('tji,tjk->tik', left, right, precision=highest)

def outer_right(left, right):
    return jnp.einsum('tij,tkj->tik', left, right, precision=highest)

def refresh(statistic, basis):
    powered = product(statistic, basis)
    factor = jnp.linalg.cholesky(inner_left(powered, powered))
    return lax.linalg.triangular_solve(factor, powered, left_side=False, lower=True, transpose_a=True)

def to_blocks(matrix):
    row_bands = ROWS // BLOCK
    col_bands = D // (BLOCK * N_MP)
    stacked = matrix.reshape(row_bands, BLOCK, N_MP, col_bands, BLOCK)
    stacked = jnp.transpose(stacked, (2, 0, 3, 1, 4)).reshape(N_MP, N_DP, TILES_DEV, BLOCK, BLOCK)
    return jnp.transpose(stacked, (1, 0, 2, 3, 4)).reshape(TILES, BLOCK, BLOCK)

def from_blocks(stacked):
    row_bands = ROWS // BLOCK
    col_bands = D // (BLOCK * N_MP)
    grouped = stacked.reshape(N_DP, N_MP, TILES_DEV, BLOCK, BLOCK)
    grouped = jnp.transpose(grouped, (1, 0, 2, 3, 4)).reshape(N_MP, row_bands, col_bands, BLOCK, BLOCK)
    return jnp.transpose(grouped, (1, 3, 0, 2, 4)).reshape(ROWS, D)

def accumulate(running, replica):
    return (running + replica.astype(jnp.float32), None)

def reference(partials, momentum, second, left_stat, right_stat, left_basis, right_basis):
    gradient, unused = lax.scan(accumulate, jnp.zeros((ROWS, D), jnp.float32), partials)
    blocks = to_blocks(gradient)
    grad_norm = jnp.sum(blocks * blocks)
    left_new = beta_second * left_stat + (1.0 - beta_second) * outer_right(blocks, blocks)
    right_new = beta_second * right_stat + (1.0 - beta_second) * inner_left(blocks, blocks)
    momentum_new = beta_first * momentum + (1.0 - beta_first) * blocks
    grad_rot = product(inner_left(left_basis, blocks), right_basis)
    moment_rot = product(inner_left(left_basis, momentum_new), right_basis)
    second_new = beta_second * second + (1.0 - beta_second) * grad_rot * grad_rot
    direction = moment_rot / (jnp.sqrt(second_new) + epsilon)
    step_norm = jnp.sum(direction * direction)
    raw_step = outer_right(product(left_basis, direction), right_basis)
    update = (raw_step * jnp.sqrt(grad_norm / step_norm)).astype(jnp.bfloat16)
    return (from_blocks(update), momentum_new, second_new, left_new, right_new, refresh(left_new, left_basis), refresh(right_new, right_basis))
```

```python
import functools

import jax
import jax.numpy as jnp
from jax import lax
from jax.experimental import pallas as pl
from jax.experimental.pallas import tpu as pltpu
from jax.sharding import Mesh
from jax.sharding import PartitionSpec as P

MESH = pl.DeviceIdType.MESH
HI = lax.Precision.HIGHEST
BLOCK = 256
HALF = 128
NB = 32

beta_first = 0.9
beta_second = 0.95
epsilon = 1e-08


def mm(a, b, ca=1, cb=0):
    return lax.dot_general(
        a, b, (((ca,), (cb,)), ((), ())), precision=HI, preferred_element_type=jnp.float32
    )


def diagonal_inverse(dl, dr, off):
    n = NB // 8
    lane = lax.broadcasted_iota(jnp.int32, (8, 128), 1)
    sub = lax.broadcasted_iota(jnp.int32, (8, 128), 0)
    is_left = lane < 64

    def row(x, s):
        return jnp.broadcast_to(x[s : s + 1, :], (8, 128))

    c = {}
    for j in range(NB):
        for v in range(j // 8, n):
            at_left = jnp.broadcast_to(dl[v][:, off + j : off + j + 1], (8, 128))
            at_right = jnp.broadcast_to(dr[v][:, off + j : off + j + 1], (8, 128))
            c[j, v] = jnp.where(is_left, at_left, at_right)
    lane64 = jnp.bitwise_and(lane, 63)
    x = [jnp.where(lane64 == sub + 8 * v, 1.0, 0.0) for v in range(n)]
    for j in range(NB):
        vj, sj = j // 8, j % 8
        r = lax.rsqrt(row(c[j, vj], sj))
        col = {v: c[j, v] * r for v in range(vj, n)}
        for k in range(j + 1, NB):
            m = row(col[k // 8], k % 8)
            for v in range(k // 8, n):
                c[k, v] = c[k, v] - col[v] * m
        xr = row(x[vj], sj) * r
        x[vj] = jnp.where(sub == sj, xr, jnp.where(sub > sj, x[vj] - col[vj] * xr, x[vj]))
        for v in range(vj + 1, n):
            x[v] = x[v] - col[v] * xr
    return jnp.concatenate(x, axis=0)


def factor_block(k, wl, wr):
    r0 = NB * k
    rows = pl.ds(r0, NB)
    first = 128 * (r0 // 128)
    off = r0 - first
    acc = []
    for w in (wl, wr):
        a = w[rows, first:]
        if k:
            a = a - mm(w[0:r0, first : first + 128], w[0:r0, first:], 0, 0)[off : off + NB]
        acc.append(a)
    groups = [[a[8 * v : 8 * v + 8, 0:128] for v in range(NB // 8)] for a in acc]
    inv = diagonal_inverse(groups[0], groups[1], off)
    for w, a, o in ((wl, acc[0], 0), (wr, acc[1], 64)):
        w[rows, first:] = mm(inv[:, o : o + NB], a)


def kernel(
    nx, nz, ny, part, mom, sec, lstat, rstat, lbas, rbas,
    upd, mom_o, sec_o, ln_o, rn_o, lb_o, rb_o,
    state, res, own, r1, pair, rsib, r2, g_ref, tmp, wl, wr, nsend, nrecv, nsum, ysend, yrecv, ublk, gath,
    s_state, s_res, s_own, s1s, s1r, sbs, sbr, s2s, s2r, nps, npr, nys, nyr, a1s, a1r, a2s, a2r, abs_, abr, s_out,
):
    x, z, c, y = (lax.axis_index(a) for a in ("x", "z", "c", "y"))
    n = (nx, nz)
    pos = (x, z)
    sib = (x, z, 1 - c, y)

    def peer(axis, d):
        return ((x + d) % nx, z, c, y) if axis == 0 else (x, (z + d) % nz, c, y)

    def ypeer(d):
        return (x, z, c, (y + d) % ny)

    def rdma(src, dst, ss, rs, dev):
        return pltpu.make_async_remote_copy(
            src_ref=src, dst_ref=dst, send_sem=ss, recv_sem=rs, device_id=dev, device_id_type=MESH
        )

    loads = [
        pltpu.make_async_copy(src, state.at[i], s_state.at[i])
        for i, src in enumerate((mom, sec, lstat, rstat, lbas, rbas))
    ]

    def slab(h, bx, bz):
        return part.at[bx, HALF * h : HALF * (h + 1), pl.ds(pl.multiple_of(512 * bz, 512), 512)]

    def chunk(h, d, e):
        if h == 0:
            return slab(0, (x + d) % nx, (z + e) % nz)
        return slab(1, (x + e) % nx, (z + d) % nz)

    order = {h: [e for e in (2, 1, 3) if e < n[1 - h]] + [0] for h in (0, 1)}
    dist = {h: [d for d in (2, 1, 3) if d < n[h]] for h in (0, 1)}
    own_copies = {
        (h, e): pltpu.make_async_copy(chunk(h, 0, e), own.at[h, e], s_own.at[h, e])
        for h in (0, 1)
        for e in order[h]
    }

    barrier = pltpu.get_barrier_semaphore()
    hello = [peer(a, d) for a in (0, 1) for d in range(1, n[a])] + [ypeer(d) for d in range(1, ny)] + [sib]
    for dev in hello:
        pl.semaphore_signal(barrier, inc=1, device_id=dev, device_id_type=MESH)
    for q in own_copies.values():
        q.start()
    for q in loads:
        q.start()
    pl.semaphore_wait(barrier, len(hello))

    phase1 = {}
    for e in range(max(nx, nz)):
        for h in (0, 1):
            if e < len(order[h]):
                ee = order[h][e]
                for d in dist[h]:
                    q = rdma(
                        chunk(h, d, ee), r1.at[h, d - 1, ee], s1s.at[h, d - 1, ee], s1r.at[h, d - 1, ee], peer(h, d)
                    )
                    q.start()
                    phase1[h, d, ee] = q

    for q in loads:
        q.wait()
    lb, rb = state[4], state[5]
    tmp[0] = beta_second * mm(lb, state[2], 0, 0)
    tmp[1] = beta_second * mm(rb, state[3], 0, 0)
    tmp[2] = beta_first * mm(mm(lb, state[0], 0, 0), rb)

    sibling, phase2 = {}, {}

    def pass_on(h, e):
        q = sibling[h, e]
        q.wait_recv()
        pair[h, c, e] = pair[h, c, e] + rsib[h, e]
        if e:
            q = rdma(pair.at[h, c, e], r2.at[h, e - 1], s2s.at[h, e - 1], s2r.at[h, e - 1], peer(1 - h, e))
            q.start()
            phase2[h, e] = q

    steps = max(len(order[0]), len(order[1]))
    for i in range(steps + 1):
        for h in (0, 1):
            if i < len(order[h]):
                e = order[h][i]
                own_copies[h, e].wait()
                for d in dist[h]:
                    phase1[h, d, e].wait_recv()
                total = own[h, e].astype(jnp.float32)
                for d in range(1, n[h]):
                    total = total + r1[h, d - 1, e].astype(jnp.float32)
                pair[h, 0, e] = total[:, :BLOCK]
                pair[h, 1, e] = total[:, BLOCK:]
                q = rdma(pair.at[h, 1 - c, e], rsib.at[h, e], sbs.at[h, e], sbr.at[h, e], sib)
                q.start()
                sibling[h, e] = q
        for h in (0, 1):
            if 1 <= i <= len(order[h]):
                pass_on(h, order[h][i - 1])
    for h in (0, 1):
        total = pair[h, c, 0]
        for e in dist[1 - h]:
            phase2[h, e].wait_recv()
            total = total + r2[h, e - 1]
        g_ref[HALF * h : HALF * (h + 1), :] = total

    g = g_ref[...]
    t1 = mm(lb, g, 0, 0)
    rot = mm(t1, rb)
    second_new = beta_second * state[1] + (1.0 - beta_second) * rot * rot
    direction = (tmp[2] + (1.0 - beta_first) * rot) / (jnp.sqrt(second_new) + epsilon)
    res[1] = second_new

    def folded(v):
        s = jnp.sum(v * v, axis=0, keepdims=True)
        return s[:, :128] + s[:, 128:]

    nsend[0:1, :] = folded(g)
    nsend[1:2, :] = folded(direction)
    members = 2 * nx * nz
    me = (x * nz + z) * 2 + c
    plane = []
    for k in range(1, members):
        to = (me + k) % members
        dev = (to // (2 * nz), (to // 2) % nz, to % 2, y)
        q = rdma(nsend, nrecv.at[k - 1], nps.at[k - 1], npr.at[k - 1], dev)
        q.start()
        plane.append(q)

    tmp[2] = mm(mm(lb, direction), rb, 1, 1)
    t2 = mm(g, rb)
    pl_t = tmp[0] + (1.0 - beta_second) * mm(t1, g, 1, 1)
    pr_t = tmp[1] + (1.0 - beta_second) * mm(t2, g, 0, 0)
    wl[:, BLOCK:] = pl_t
    wr[:, BLOCK:] = pr_t
    wl[:, :BLOCK] = mm(pl_t, pl_t, 1, 1)
    wr[:, :BLOCK] = mm(pr_t, pr_t, 1, 1)
    res[0] = beta_first * state[0] + (1.0 - beta_first) * g
    res[2] = beta_second * state[2] + (1.0 - beta_second) * mm(g, g, 1, 1)
    res[3] = beta_second * state[3] + (1.0 - beta_second) * mm(g, g, 0, 0)
    stores = [
        pltpu.make_async_copy(res.at[i], dst, s_res.at[i])
        for i, dst in enumerate((mom_o, sec_o, ln_o, rn_o, lb_o, rb_o))
    ]
    for q in stores[:4]:
        q.start()

    blocks = BLOCK // NB
    factor_block(0, wl, wr)

    for q in plane:
        q.wait_recv()
    total = nsend[...]
    for k in range(members - 1):
        total = total + nrecv[k]
    ysend[...] = total
    along_y = []
    for d in range(1, ny):
        q = rdma(ysend, yrecv.at[d - 1], nys.at[d - 1], nyr.at[d - 1], ypeer(d))
        q.start()
        along_y.append(q)

    factor_block(1, wl, wr)
    factor_block(2, wl, wr)

    for q in along_y:
        q.wait_recv()
    total = ysend[...]
    for d in range(1, ny):
        total = total + yrecv[d - 1]
    sums = jnp.sum(total, axis=1, keepdims=True)
    scale = jnp.sqrt(sums[0:1, :] / sums[1:2, :])
    ublk[...] = (tmp[2] * scale).astype(jnp.bfloat16)

    def place(h, bx, bz):
        return upd.at[bx, HALF * h : HALF * (h + 1), pl.ds(pl.multiple_of(512 * bz + 256 * c, 256), 256)]

    def held(h, s):
        return ublk.at[HALF * h : HALF * (h + 1), :] if s == 0 else gath.at[h, s - 1]

    def source(h, s):
        return place(h, x, (z + nz - s) % nz) if h == 0 else place(h, (x + nx - s) % nx, z)

    def arrived(h, d, s):
        if h == 0:
            return place(h, (x + nx - d) % nx, (z + nz - s) % nz)
        return place(h, (x + nx - s) % nx, (z + nz - d) % nz)

    ag1, ag2, to_sib, local = {}, {}, [], []

    def forward(h, s):
        for d in dist[h]:
            q = rdma(held(h, s), source(h, s), a2s.at[h, d - 1, s], a2r.at[h, d - 1, s], peer(h, d))
            q.start()
            ag2[h, d, s] = q
        i = len(to_sib)
        q = rdma(held(h, s), source(h, s), abs_.at[i], abr.at[i], sib)
        q.start()
        to_sib.append(q)
        q = pltpu.make_async_copy(held(h, s), source(h, s), s_out.at[h, s])
        q.start()
        local.append(q)

    for h in (0, 1):
        for d in dist[1 - h]:
            q = rdma(held(h, 0), gath.at[h, d - 1], a1s.at[h, d - 1], a1r.at[h, d - 1], peer(1 - h, d))
            q.start()
            ag1[h, d] = q
    for h in (0, 1):
        forward(h, 0)

    factor_block(3, wl, wr)
    factor_block(4, wl, wr)

    for s in (1, 3, 2):
        for h in (0, 1):
            if s < n[1 - h]:
                ag1[h, s].wait_recv()
                forward(h, s)

    for k in range(5, blocks):
        factor_block(k, wl, wr)
    res[4] = wl[:, BLOCK:].T
    res[5] = wr[:, BLOCK:].T
    for q in stores[4:]:
        q.start()

    for s in (0, 1, 3, 2):
        for d in (1, 3, 2):
            for h in (0, 1):
                if d < n[h] and s < n[1 - h]:
                    ag2[h, d, s].wait_recv()
                    i = len(to_sib)
                    q = rdma(arrived(h, d, s), arrived(h, d, s), abs_.at[i], abr.at[i], sib)
                    q.start()
                    to_sib.append(q)

    for q in to_sib:
        q.wait_recv()
    for q in local + stores:
        q.wait()
    for group in (phase1, sibling, phase2, ag1, ag2):
        for q in group.values():
            q.wait_send()
    for q in plane + along_y + to_sib:
        q.wait_send()


def on_device(nx, nz, ny, partials, *states):
    f32, bf16 = jnp.float32, jnp.bfloat16
    rows, width = partials.shape[1:]
    part = partials.reshape(nx, BLOCK, width)
    hbm = pl.BlockSpec(memory_space=pl.ANY)
    ring = max(nx, nz)
    square = (BLOCK, BLOCK)
    dma = pltpu.SemaphoreType.DMA
    members = 2 * nx * nz
    blocks = 2 * nx * nz
    outs = pl.pallas_call(
        functools.partial(kernel, nx, nz, ny),
        out_shape=[jax.ShapeDtypeStruct((nx, BLOCK, width), bf16)] + [jax.ShapeDtypeStruct(square, f32)] * 6,
        in_specs=[hbm] * 7,
        out_specs=[hbm] * 7,
        scratch_shapes=[
            pltpu.VMEM((6, *square), f32),
            pltpu.VMEM((6, *square), f32),
            pltpu.VMEM((2, ring, HALF, 2 * BLOCK), bf16),
            pltpu.VMEM((2, ring - 1, ring, HALF, 2 * BLOCK), bf16),
            pltpu.VMEM((2, 2, ring, HALF, BLOCK), f32),
            pltpu.VMEM((2, ring, HALF, BLOCK), f32),
            pltpu.VMEM((2, ring - 1, HALF, BLOCK), f32),
            pltpu.VMEM(square, f32),
            pltpu.VMEM((3, *square), f32),
            pltpu.VMEM((BLOCK, 2 * BLOCK), f32),
            pltpu.VMEM((BLOCK, 2 * BLOCK), f32),
            pltpu.VMEM((2, 128), f32),
            pltpu.VMEM((members - 1, 2, 128), f32),
            pltpu.VMEM((2, 128), f32),
            pltpu.VMEM((2, 128), f32),
            pltpu.VMEM((ny - 1, 2, 128), f32),
            pltpu.VMEM(square, bf16),
            pltpu.VMEM((2, ring - 1, HALF, BLOCK), bf16),
            dma((6,)), dma((6,)), dma((2, ring)),
            dma((2, ring - 1, ring)), dma((2, ring - 1, ring)),
            dma((2, ring)), dma((2, ring)),
            dma((2, ring - 1)), dma((2, ring - 1)),
            dma((members - 1,)), dma((members - 1,)),
            dma((ny - 1,)), dma((ny - 1,)),
            dma((2, ring - 1)), dma((2, ring - 1)),
            dma((2, ring - 1, ring)), dma((2, ring - 1, ring)),
            dma((blocks,)), dma((blocks,)),
            dma((2, ring)),
        ],
        compiler_params=pltpu.CompilerParams(
            collective_id=0, has_side_effects=True, vmem_limit_bytes=48 * 1024 * 1024
        ),
    )(part, *(s[0] for s in states))
    return (outs[0].reshape(rows, width), *(o[None] for o in outs[1:]))


def solution(mesh):
    nx = nz = 4
    ny = mesh.shape["mp"]
    split = Mesh(mesh.devices.reshape(nx, nz, 2, ny), ("x", "z", "c", "y"))
    dp = ("x", "z", "c")
    whole = P(dp + ("y",), None, None)
    return jax.shard_map(
        functools.partial(on_device, nx, nz, ny),
        mesh=split,
        in_specs=(P(dp, None, "y"),) + (whole,) * 6,
        out_specs=(P(None, "y"),) + (whole,) * 6,
        check_vma=False,
    )
```

```python
import functools

import jax
import jax.numpy as jnp
from jax import lax
from jax.experimental import pallas as pl
from jax.experimental.pallas import tpu as pltpu
from jax.sharding import Mesh
from jax.sharding import PartitionSpec as P

MESH = pl.DeviceIdType.MESH
HI = lax.Precision.HIGHEST
BLOCK = 256
HALF = 128
NB = 32
EARLY = 3

beta_first = 0.9
beta_second = 0.95
epsilon = 1e-08


def mm(a, b, ca=1, cb=0):
    return lax.dot_general(
        a, b, (((ca,), (cb,)), ((), ())), precision=HI, preferred_element_type=jnp.float32
    )


def parts(a):
    high = a.astype(jnp.bfloat16)
    return high, (a - high.astype(jnp.float32)).astype(jnp.bfloat16)


def mm3(a, b, ca=1, cb=0):
    dot = lambda u, v: lax.dot_general(u, v, (((ca,), (cb,)), ((), ())), preferred_element_type=jnp.float32)
    return dot(a[0], b[0]) + (dot(a[0], b[1]) + dot(a[1], b[0]))


def diagonal_inverse(dl, dr, off):
    n = NB // 8
    lane = lax.broadcasted_iota(jnp.int32, (8, 128), 1)
    sub = lax.broadcasted_iota(jnp.int32, (8, 128), 0)
    is_left = lane < 64

    def row(x, s):
        return jnp.broadcast_to(x[s : s + 1, :], (8, 128))

    c = {}
    for j in range(NB):
        for v in range(j // 8, n):
            at_left = jnp.broadcast_to(dl[v][:, off + j : off + j + 1], (8, 128))
            at_right = jnp.broadcast_to(dr[v][:, off + j : off + j + 1], (8, 128))
            c[j, v] = jnp.where(is_left, at_left, at_right)
    lane64 = jnp.bitwise_and(lane, 63)
    x = [jnp.where(lane64 == sub + 8 * v, 1.0, 0.0) for v in range(n)]
    for j in range(NB):
        vj, sj = j // 8, j % 8
        r = lax.rsqrt(row(c[j, vj], sj))
        col = {v: c[j, v] * r for v in range(vj, n)}
        for k in range(j + 1, NB):
            m = row(col[k // 8], k % 8)
            for v in range(k // 8, n):
                c[k, v] = c[k, v] - col[v] * m
        xr = row(x[vj], sj) * r
        x[vj] = jnp.where(sub == sj, xr, jnp.where(sub > sj, x[vj] - col[vj] * xr, x[vj]))
        for v in range(vj + 1, n):
            x[v] = x[v] - col[v] * xr
    return jnp.concatenate(x, axis=0)


def factor_block(k, wl, wr):
    r0 = NB * k
    rows = pl.ds(r0, NB)
    first = 128 * (r0 // 128)
    off = r0 - first
    acc = []
    for w in (wl, wr):
        a = w[rows, first:]
        if k:
            a = a - mm(w[0:r0, first : first + 128], w[0:r0, first:], 0, 0)[off : off + NB]
        acc.append(a)
    groups = [[a[8 * v : 8 * v + 8, 0:128] for v in range(NB // 8)] for a in acc]
    inv = diagonal_inverse(groups[0], groups[1], off)
    for w, a, o in ((wl, acc[0], 0), (wr, acc[1], 64)):
        w[rows, first:] = mm(inv[:, o : o + NB], a)


def kernel(
    nx, nz, ny, part, mom, sec, lstat, rstat, lbas, rbas,
    upd, mom_o, sec_o, ln_o, rn_o, lb_o, rb_o,
    state, own, r1, pair, rsib, r2, g_ref, tmp, wl, wr, nsend, nrecv,
    s_state, s_own, s1s, s1r, sbs, sbr, s2s, s2r, nps, npr, a1s, a1r, a2s, a2r, abs_, abr,
):
    x, z, c, y = (lax.axis_index(a) for a in ("x", "z", "c", "y"))
    n = (nx, nz)
    xs = [x] + [(x + d) % nx for d in range(1, nx)]
    zs = [z] + [(z + d) % nz for d in range(1, nz)]
    ys = [y] + [(y + d) % ny for d in range(1, ny)]
    cs = [c, 1 - c]
    sib = (x, z, cs[1], y)

    def peer(axis, d):
        return (xs[d], z, c, y) if axis == 0 else (x, zs[d], c, y)

    def rdma(src, dst, ss, rs, dev):
        return pltpu.make_async_remote_copy(
            src_ref=src, dst_ref=dst, send_sem=ss, recv_sem=rs, device_id=dev, device_id_type=MESH
        )

    def bytes_of(ref, sem):
        pltpu.make_async_copy(ref, ref, sem).wait()

    loads = [
        pltpu.make_async_copy(src, state.at[i], s_state.at[i])
        for i, src in enumerate((mom, sec, lstat, rstat, lbas, rbas))
    ]

    def slab(h, bx, bz):
        return part.at[bx, HALF * h : HALF * (h + 1), pl.ds(pl.multiple_of(512 * bz, 512), 512)]

    def chunk(h, d, e):
        return slab(0, xs[d], zs[e]) if h == 0 else slab(1, xs[e], zs[d])

    order = {h: [e for e in (2, 1, 3) if e < n[1 - h]] + [0] for h in (0, 1)}
    dist = {h: [d for d in (2, 1, 3) if d < n[h]] for h in (0, 1)}
    own_copies = {
        (h, e): pltpu.make_async_copy(chunk(h, 0, e), own.at[h, e], s_own.at[h, e])
        for h in (0, 1)
        for e in order[h]
    }

    barrier = pltpu.get_barrier_semaphore()
    hello = [peer(a, d) for a in (0, 1) for d in range(1, n[a])] + [(x, z, c, v) for v in ys[1:]] + [sib]
    for dev in hello:
        pl.semaphore_signal(barrier, inc=1, device_id=dev, device_id_type=MESH)
    for q in own_copies.values():
        q.start()
    for q in loads:
        q.start()
    pl.semaphore_wait(barrier, len(hello))

    for i in range(max(nx, nz)):
        for h in (0, 1):
            if i < len(order[h]):
                e = order[h][i]
                for d in dist[h]:
                    rdma(chunk(h, d, e), r1.at[h, e, d - 1], s1s.at[0], s1r.at[h, e], peer(h, d)).start()

    for q in loads:
        q.wait()
    lb, rb = state[4], state[5]
    lbt, rbt = lb.T, rb.T
    tmp[0] = beta_second * mm(lbt, state[2])
    tmp[1] = beta_second * mm(rbt, state[3])
    tmp[2] = beta_first * mm(mm(lbt, state[0]), rb)
    tmp[3] = lbt
    tmp[4] = rbt

    def pass_on(h, e):
        bytes_of(rsib.at[h, e], sbr.at[h, e])
        pair[h, c, e] = pair[h, c, e] + rsib[h, e]
        if e:
            rdma(pair.at[h, c, e], r2.at[h, e - 1], s2s.at[0], s2r.at[h], peer(1 - h, e)).start()

    for i in range(max(nx, nz) + 1):
        for h in (0, 1):
            if i < len(order[h]):
                e = order[h][i]
                own_copies[h, e].wait()
                bytes_of(r1.at[h, e], s1r.at[h, e])
                total = own[h, e].astype(jnp.float32)
                for d in range(1, n[h]):
                    total = total + r1[h, e, d - 1].astype(jnp.float32)
                pair[h, 0, e] = total[:, :BLOCK]
                pair[h, 1, e] = total[:, BLOCK:]
                rdma(pair.at[h, cs[1], e], rsib.at[h, e], sbs.at[0], sbr.at[h, e], sib).start()
        for h in (0, 1):
            if 1 <= i <= len(order[h]):
                pass_on(h, order[h][i - 1])
    for h in (0, 1):
        total = pair[h, c, 0]
        bytes_of(r2.at[h], s2r.at[h])
        for e in range(1, n[1 - h]):
            total = total + r2[h, e - 1]
        g_ref[HALF * h : HALF * (h + 1), :] = total

    g = g_ref[...]
    gp, rbp = parts(g), parts(rb)
    t1p = parts(mm3(parts(tmp[3]), gp))
    rot = mm3(t1p, rbp)
    second_new = beta_second * state[1] + (1.0 - beta_second) * rot * rot
    direction = (tmp[2] + (1.0 - beta_first) * rot) / (jnp.sqrt(second_new) + epsilon)
    sec_o[...] = second_new

    def folded(v):
        s = jnp.sum(v * v, axis=0, keepdims=True)
        s = s[:, :128] + s[:, 128:]
        return s + pltpu.roll(s, 64, 1)

    is_grad = lax.broadcasted_iota(jnp.int32, (1, 128), 1) < 64
    mine = jnp.where(is_grad, folded(g), folded(direction))
    nsend[...] = mine
    others = 2 * nx * nz * ny - 1
    for dx in range(nx):
        for dz in range(nz):
            for dc in range(2):
                for dy in range(ny):
                    k = ((dx * nz + dz) * 2 + dc) * ny + dy
                    if k:
                        dev = (xs[dx], zs[dz], cs[dc], ys[dy])
                        rdma(nsend, nrecv.at[k - 1 : k, :], nps.at[0], npr.at[0], dev).start()

    tmp[2] = mm3(parts(mm3(parts(lb), parts(direction))), rbp, 1, 1)
    t2p = parts(mm3(parts(tmp[4]), gp, 1, 1))
    pl_t = tmp[0] + (1.0 - beta_second) * mm3(t1p, gp, 1, 1)
    pr_t = tmp[1] + (1.0 - beta_second) * mm3(t2p, gp)
    wl[:, BLOCK:] = pl_t
    wr[:, BLOCK:] = pr_t
    wl[:, :BLOCK] = mm(pl_t, pl_t, 1, 1)
    wr[:, :BLOCK] = mm(pr_t, pr_t, 1, 1)
    for k in range(EARLY):
        factor_block(k, wl, wr)

    bytes_of(nrecv.at[0:others, :], npr.at[0])
    total = jnp.sum(nrecv[0:others, :], axis=0, keepdims=True) + mine
    grad_norm = jnp.sum(jnp.where(is_grad, total, 0.0), axis=1, keepdims=True)
    step_norm = jnp.sum(jnp.where(is_grad, 0.0, total), axis=1, keepdims=True)
    update = (tmp[2] * jnp.sqrt(grad_norm / step_norm)).astype(jnp.bfloat16)
    columns = pl.ds(pl.multiple_of(512 * z + 256 * c, 256), 256)
    upd[x, :, columns] = update

    def place(h, bx, bz):
        return upd.at[bx, HALF * h : HALF * (h + 1), pl.ds(pl.multiple_of(512 * bz + 256 * c, 256), 256)]

    def spot(h, d, s):
        back = lambda v, k, m: v[(m - k) % m]
        return place(h, back(xs, d, nx), back(zs, s, nz)) if h == 0 else place(h, back(xs, s, nx), back(zs, d, nz))

    def send(where, ss, rs, dev):
        rdma(where, where, ss, rs, dev).start()

    def arrive(where, rs):
        bytes_of(where, rs)

    def share(h, d, s):
        send(spot(h, d, s), abs_.at[0], abr.at[0], sib)

    def start(h):
        for d in (1, 3, 2):
            send(spot(h, 0, 0), a1s.at[0], a1r.at[h, d - 1], peer(1 - h, d))

    def onward(h, s):
        if s:
            arrive(spot(h, 0, s), a1r.at[h, s - 1])
        for d in (2, 1, 3) if s == 2 else (1, 3):
            send(spot(h, 0, s), a2s.at[0], a2r.at[h, d - 1, s], peer(h, d))
        share(h, 0, s)

    ways = {0: 1, 1: 3, 3: 1}

    def relay(h, s):
        for d in (1, 3):
            arrive(spot(h, d, s), a2r.at[h, d - 1, s])
            if ways.get(s) == d:
                send(spot(h, d, s), a2s.at[0], a2r.at[h, 1, s], peer(h, d))
            share(h, d, s)

    def last(h, s):
        arrive(spot(h, 2, s), a2r.at[h, 1, s])
        share(h, 2, s)

    both = lambda f, *a: [f(h, *a) for h in (0, 1)]
    both(start)
    both(onward, 0)

    def rest_of_products():
        mom_o[...] = beta_first * state[0] + (1.0 - beta_first) * g_ref[...]
        q = parts(g_ref[...])
        ln_o[...] = beta_second * state[2] + (1.0 - beta_second) * mm3(q, q, 1, 1)
        qt = parts(g_ref[...].T)
        rn_o[...] = beta_second * state[3] + (1.0 - beta_second) * mm3(qt, q)

    def bases():
        lb_o[...] = wl[:, BLOCK:].T
        rb_o[...] = wr[:, BLOCK:].T

    work = [functools.partial(factor_block, k, wl, wr) for k in range(EARLY, BLOCK // NB)]
    work = work + [rest_of_products, bases]
    polls = {
        1: ((onward, 1), (onward, 3)),
        2: ((relay, 0), (onward, 2)),
        3: ((relay, 1),),
        4: ((last, 0), (relay, 3)),
        5: ((last, 1), (relay, 2)),
        len(work) - 1: ((last, 3), (last, 2)),
    }
    for i, do in enumerate(work):
        do()
        for q in polls.get(i, ()):
            both(*q)

    bytes_of(upd.at[0:2], abr.at[0])
    bytes_of(r1, s1s.at[0])
    bytes_of(rsib, sbs.at[0])
    bytes_of(r2, s2s.at[0])
    bytes_of(nrecv.at[0:others, :], nps.at[0])
    bytes_of(upd.at[0, 0:192, 0:1024], a1s.at[0])
    bytes_of(upd.at[0:3, 0:128, :], a2s.at[0])
    bytes_of(upd.at[0:2], abs_.at[0])


def store_kernel(*refs):
    m = len(refs) // 2
    sem = refs[-1]
    copies = [pltpu.make_async_copy(refs[i], refs[m + i], sem.at[i]) for i in range(m)]
    for q in copies:
        q.start()
    for q in copies:
        q.wait()


def on_device(nx, nz, ny, partials, *states):
    f32, bf16 = jnp.float32, jnp.bfloat16
    rows, width = partials.shape[1:]
    part = partials.reshape(nx, BLOCK, width)
    hbm = pl.BlockSpec(memory_space=pltpu.HBM)
    vmem = pl.BlockSpec(memory_space=pltpu.VMEM)
    ring = max(nx, nz)
    square = (BLOCK, BLOCK)
    dma = pltpu.SemaphoreType.DMA
    members = 2 * nx * nz
    shapes = [jax.ShapeDtypeStruct((nx, BLOCK, width), bf16)] + [jax.ShapeDtypeStruct(square, f32)] * 6
    outs = pl.pallas_call(
        functools.partial(kernel, nx, nz, ny),
        out_shape=shapes,
        in_specs=[hbm] * 7,
        out_specs=[vmem] * 7,
        scratch_shapes=[
            pltpu.VMEM((6, *square), f32),
            pltpu.VMEM((2, ring, HALF, 2 * BLOCK), bf16),
            pltpu.VMEM((2, ring, ring - 1, HALF, 2 * BLOCK), bf16),
            pltpu.VMEM((2, 2, ring, HALF, BLOCK), f32),
            pltpu.VMEM((2, ring, HALF, BLOCK), f32),
            pltpu.VMEM((2, ring - 1, HALF, BLOCK), f32),
            pltpu.VMEM(square, f32),
            pltpu.VMEM((5, *square), f32),
            pltpu.VMEM((BLOCK, 2 * BLOCK), f32),
            pltpu.VMEM((BLOCK, 2 * BLOCK), f32),
            pltpu.VMEM((1, 128), f32),
            pltpu.VMEM((members * ny, 128), f32),
            dma((6,)), dma((2, ring)),
            dma((1,)), dma((2, ring)),
            dma((1,)), dma((2, ring)),
            dma((1,)), dma((2,)),
            dma((1,)), dma((1,)),
            dma((1,)), dma((2, ring - 1)),
            dma((1,)), dma((2, ring - 1, ring)),
            dma((1,)), dma((1,)),
        ],
        compiler_params=pltpu.CompilerParams(
            collective_id=0, has_side_effects=True, vmem_limit_bytes=36 * 1024 * 1024
        ),
    )(*(pltpu.with_memory_space_constraint(a, pltpu.HBM) for a in (part, *(s[0] for s in states))))
    outs = pl.pallas_call(
        store_kernel,
        out_shape=shapes,
        in_specs=[vmem] * 7,
        out_specs=[hbm] * 7,
        scratch_shapes=[dma((7,))],
        compiler_params=pltpu.CompilerParams(vmem_limit_bytes=8 * 1024 * 1024),
    )(*outs)
    return (outs[0].reshape(rows, width), *(o[None] for o in outs[1:]))


def solution(mesh):
    nx = nz = 4
    ny = mesh.shape["mp"]
    split = Mesh(mesh.devices.reshape(nx, nz, 2, ny), ("x", "z", "c", "y"))
    dp = ("x", "z", "c")
    whole = P(dp + ("y",), None, None)
    return jax.shard_map(
        functools.partial(on_device, nx, nz, ny),
        mesh=split,
        in_specs=(P(dp, None, "y"),) + (whole,) * 6,
        out_specs=(P(None, "y"),) + (whole,) * 6,
        check_vma=False,
    )
```

```python
import functools

import jax
import jax.numpy as jnp
from jax import lax
from jax.experimental import pallas as pl
from jax.experimental.pallas import tpu as pltpu
from jax.sharding import Mesh
from jax.sharding import PartitionSpec as P

MESH = pl.DeviceIdType.MESH
HI = lax.Precision.HIGHEST
BLOCK = 256
HALF = 128
QUART = 64
NB = 32
EARLY = 2

beta_first = 0.9
beta_second = 0.95
epsilon = 1e-08


def mm(a, b, ca=1, cb=0):
    return lax.dot_general(
        a, b, (((ca,), (cb,)), ((), ())), precision=HI, preferred_element_type=jnp.float32
    )


def parts(a):
    high = a.astype(jnp.bfloat16)
    return high, (a - high.astype(jnp.float32)).astype(jnp.bfloat16)


def mm3(a, b, ca=1, cb=0):
    dot = lambda u, v: lax.dot_general(u, v, (((ca,), (cb,)), ((), ())), preferred_element_type=jnp.float32)
    return dot(a[0], b[0]) + (dot(a[0], b[1]) + dot(a[1], b[0]))


def diagonal_inverse(dl, dr, off):
    n = NB // 8
    lane = lax.broadcasted_iota(jnp.int32, (8, 128), 1)
    sub = lax.broadcasted_iota(jnp.int32, (8, 128), 0)
    is_left = lane < 64

    def row(x, s):
        return jnp.broadcast_to(x[s : s + 1, :], (8, 128))

    c = {}
    for j in range(NB):
        for v in range(j // 8, n):
            at_left = jnp.broadcast_to(dl[v][:, off + j : off + j + 1], (8, 128))
            at_right = jnp.broadcast_to(dr[v][:, off + j : off + j + 1], (8, 128))
            c[j, v] = jnp.where(is_left, at_left, at_right)
    lane64 = jnp.bitwise_and(lane, 63)
    x = [jnp.where(lane64 == sub + 8 * v, 1.0, 0.0) for v in range(n)]
    for j in range(NB):
        vj, sj = j // 8, j % 8
        r = lax.rsqrt(row(c[j, vj], sj))
        col = {v: c[j, v] * r for v in range(vj, n)}
        for k in range(j + 1, NB):
            m = row(col[k // 8], k % 8)
            for v in range(k // 8, n):
                c[k, v] = c[k, v] - col[v] * m
        xr = row(x[vj], sj) * r
        x[vj] = jnp.where(sub == sj, xr, jnp.where(sub > sj, x[vj] - col[vj] * xr, x[vj]))
        for v in range(vj + 1, n):
            x[v] = x[v] - col[v] * xr
    return jnp.concatenate(x, axis=0)


def factor_block(k, wl, wr):
    r0 = NB * k
    rows = pl.ds(r0, NB)
    first = 128 * (r0 // 128)
    off = r0 - first
    acc = []
    for w in (wl, wr):
        a = w[rows, first:]
        if k:
            a = a - mm(w[0:r0, first : first + 128], w[0:r0, first:], 0, 0)[off : off + NB]
        acc.append(a)
    groups = [[a[8 * v : 8 * v + 8, 0:128] for v in range(NB // 8)] for a in acc]
    inv = diagonal_inverse(groups[0], groups[1], off)
    for w, a, o in ((wl, acc[0], 0), (wr, acc[1], 64)):
        w[rows, first:] = mm(inv[:, o : o + NB], a)


def kernel(
    nx, nz, ny, part, mom, sec, lstat, rstat, lbas, rbas,
    upd, mom_o, sec_o, ln_o, rn_o, lb_o, rb_o,
    state, own, f1, mid, msib, s2, r1, pair, rsib, f3, r2, g_ref, tmp, wl, wr, nsend, nrecv,
    s_state, s_own, f1s, f1r, mss, msr, s2s, s2r, s1s, s1r, sbs, sbr, f3s, f3r, s3s, s3r,
    nps, npr, a1s, a1r, a2s, a2r, abs_, abr,
):
    x, z, c, y = (lax.axis_index(a) for a in ("x", "z", "c", "y"))
    n = (nx, nz)
    xs = [x] + [(x + d) % nx for d in range(1, nx)]
    zs = [z] + [(z + d) % nz for d in range(1, nz)]
    ys = [y] + [(y + d) % ny for d in range(1, ny)]
    cs = [c, 1 - c]
    sib = (x, z, cs[1], y)

    def peer(axis, d):
        return (xs[d], z, c, y) if axis == 0 else (x, zs[d], c, y)

    def rdma(src, dst, ss, rs, dev):
        return pltpu.make_async_remote_copy(
            src_ref=src, dst_ref=dst, send_sem=ss, recv_sem=rs, device_id=dev, device_id_type=MESH
        )

    def bytes_of(ref, sem):
        pltpu.make_async_copy(ref, ref, sem).wait()

    loads = [
        pltpu.make_async_copy(src, state.at[i], s_state.at[i])
        for i, src in enumerate((mom, sec, lstat, rstat, lbas, rbas))
    ]

    def chunk(h, d, e, r0=0, rows=HALF):
        bx, bz = (xs[d], zs[e]) if h == 0 else (xs[e], zs[d])
        r0 = HALF * h + r0
        return part.at[bx, r0 : r0 + rows, pl.ds(pl.multiple_of(512 * bz, 512), 512)]

    order = (2, 1, 3, 0)
    ways = ((1, 0), (3, QUART))
    own_copies = {
        (h, e): [
            pltpu.make_async_copy(src, own.at[h, e, at : at + rows], s_own.at[h, e])
            for src, at, rows in (
                (chunk(h, 0, e), 0, HALF),
                (chunk(h, 1, e, 0, QUART), HALF, QUART),
                (chunk(h, 3, e, QUART, QUART), HALF + QUART, QUART),
            )
        ]
        for e in order
        for h in (0, 1)
    }

    barrier = pltpu.get_barrier_semaphore()
    hello = [peer(a, d) for a in (0, 1) for d in range(1, n[a])] + [(x, z, c, v) for v in ys[1:]] + [sib]
    for dev in hello:
        pl.semaphore_signal(barrier, inc=1, device_id=dev, device_id_type=MESH)
    for e in order:
        for h in (0, 1):
            for q in own_copies[h, e]:
                q.start()
    for q in loads:
        q.start()
    pl.semaphore_wait(barrier, len(hello))

    both = lambda f, *a: [f(h, *a) for h in (0, 1)]

    def send_far(h, e):
        for t, (d, r0) in enumerate(ways):
            rdma(chunk(h, 2, e, r0, QUART), f1.at[h, e, t], f1s.at[0], f1r.at[h, e], peer(h, d)).start()

    def send_near(h, e):
        for t, (d, r0) in enumerate(ways):
            rdma(chunk(h, d, e, QUART - r0, QUART), r1.at[h, e, t], s1s.at[0], s1r.at[h, e], peer(h, d)).start()

    def add_far(h, e):
        bytes_of(own.at[h, e], s_own.at[h, e])
        bytes_of(f1.at[h, e], f1r.at[h, e])
        for t in (0, 1):
            at = HALF + QUART * t
            total = own[h, e, at : at + QUART].astype(jnp.float32) + f1[h, e, t].astype(jnp.float32)
            mid[h, e, 0, t] = total[:, :BLOCK]
            mid[h, e, 1, t] = total[:, BLOCK:]
        rdma(mid.at[h, e, cs[1]], msib.at[h, e], mss.at[0], msr.at[h, e], sib).start()

    def send_sum(h, e):
        bytes_of(msib.at[h, e], msr.at[h, e])
        mid[h, e, c] = mid[h, e, c] + msib[h, e]
        for t, (d, r0) in enumerate(ways):
            rdma(mid.at[h, e, c, t], s2.at[h, e, t], s2s.at[0], s2r.at[h, e], peer(h, d)).start()

    def add_near(h, e):
        bytes_of(r1.at[h, e], s1r.at[h, e])
        for t in (0, 1):
            r0 = QUART * t
            total = own[h, e, r0 : r0 + QUART].astype(jnp.float32) + r1[h, e, 1 - t].astype(jnp.float32)
            pair[h, 0, e, t] = total[:, :BLOCK]
            pair[h, 1, e, t] = total[:, BLOCK:]
        rdma(pair.at[h, cs[1], e], rsib.at[h, e], sbs.at[0], sbr.at[h, e], sib).start()

    def pass_on(h, e):
        bytes_of(rsib.at[h, e], sbr.at[h, e])
        bytes_of(s2.at[h, e], s2r.at[h, e])
        pair[h, c, e] = pair[h, c, e] + (rsib[h, e] + s2[h, e])
        if e == 2:
            for t, (d, r0) in enumerate(ways):
                rdma(pair.at[h, c, e, t], f3.at[h, t], f3s.at[0], f3r.at[h, t], peer(1 - h, d)).start()
        elif e:
            t = 0 if e == 1 else 1
            bytes_of(f3.at[h, t], f3r.at[h, t])
            pair[h, c, e, t] = pair[h, c, e, t] + f3[h, t]
            rdma(pair.at[h, c, e], r2.at[h, t], s3s.at[0], s3r.at[h], peer(1 - h, e)).start()

    for e in order:
        both(send_far, e)
    both(send_near, 2)

    for q in loads:
        q.wait()
    lb, rb = state[4], state[5]
    lbt, rbt = lb.T, rb.T
    tmp[3] = lbt
    tmp[4] = rbt

    both(add_far, 2)
    both(add_far, 1)
    both(send_sum, 2)
    both(send_near, 1)
    both(add_far, 3)
    both(send_sum, 1)
    both(send_near, 3)
    both(add_far, 0)
    both(send_sum, 3)
    both(send_near, 0)
    both(send_sum, 0)

    tmp[0] = beta_second * mm(lbt, state[2])
    tmp[1] = beta_second * mm(rbt, state[3])
    both(add_near, 2)
    tmp[2] = beta_first * mm(mm(lbt, state[0]), rb)
    both(pass_on, 2)
    both(add_near, 1)
    both(pass_on, 1)
    both(add_near, 3)
    both(pass_on, 3)
    both(add_near, 0)
    both(pass_on, 0)
    for h in (0, 1):
        bytes_of(r2.at[h], s3r.at[h])
        for t in (0, 1):
            r0 = HALF * h + QUART * t
            g_ref[r0 : r0 + QUART, :] = pair[h, c, 0, t] + (
                r2[h, 0, t] + r2[h, 1, t]
            )

    g = g_ref[...]
    gp, rbp = parts(g), parts(rb)
    t1p = parts(mm3(parts(tmp[3]), gp))
    rot = mm3(t1p, rbp)
    second_new = beta_second * state[1] + (1.0 - beta_second) * rot * rot
    direction = (tmp[2] + (1.0 - beta_first) * rot) / (jnp.sqrt(second_new) + epsilon)
    sec_o[...] = second_new

    def folded(v):
        s = jnp.sum(v * v, axis=0, keepdims=True)
        s = s[:, :128] + s[:, 128:]
        return s + pltpu.roll(s, 64, 1)

    is_grad = lax.broadcasted_iota(jnp.int32, (1, 128), 1) < 64
    mine = jnp.where(is_grad, folded(g), folded(direction))
    nsend[...] = mine
    others = 2 * nx * nz * ny - 1
    for dx in range(nx):
        for dz in range(nz):
            for dc in range(2):
                for dy in range(ny):
                    k = ((dx * nz + dz) * 2 + dc) * ny + dy
                    if k:
                        dev = (xs[dx], zs[dz], cs[dc], ys[dy])
                        rdma(nsend, nrecv.at[k - 1 : k, :], nps.at[0], npr.at[0], dev).start()

    tmp[2] = mm3(parts(mm3(parts(lb), parts(direction))), rbp, 1, 1)
    t2p = parts(mm3(parts(tmp[4]), gp, 1, 1))
    pl_t = tmp[0] + (1.0 - beta_second) * mm3(t1p, gp, 1, 1)
    pr_t = tmp[1] + (1.0 - beta_second) * mm3(t2p, gp)
    wl[:, BLOCK:] = pl_t
    wr[:, BLOCK:] = pr_t
    wl[:, :BLOCK] = mm(pl_t, pl_t, 1, 1)
    wr[:, :BLOCK] = mm(pr_t, pr_t, 1, 1)
    for k in range(EARLY):
        factor_block(k, wl, wr)

    bytes_of(nrecv.at[0:others, :], npr.at[0])
    total = jnp.sum(nrecv[0:others, :], axis=0, keepdims=True) + mine
    grad_norm = jnp.sum(jnp.where(is_grad, total, 0.0), axis=1, keepdims=True)
    step_norm = jnp.sum(jnp.where(is_grad, 0.0, total), axis=1, keepdims=True)
    update = (tmp[2] * jnp.sqrt(grad_norm / step_norm)).astype(jnp.bfloat16)
    columns = pl.ds(pl.multiple_of(512 * z + 256 * c, 256), 256)
    upd[x, :, columns] = update

    def place(h, bx, bz):
        return upd.at[bx, HALF * h : HALF * (h + 1), pl.ds(pl.multiple_of(512 * bz + 256 * c, 256), 256)]

    def spot(h, d, s):
        back = lambda v, k, m: v[(m - k) % m]
        return place(h, back(xs, d, nx), back(zs, s, nz)) if h == 0 else place(h, back(xs, s, nx), back(zs, d, nz))

    def send(where, ss, rs, dev):
        rdma(where, where, ss, rs, dev).start()

    def arrive(where, rs):
        bytes_of(where, rs)

    def share(h, d, s):
        send(spot(h, d, s), abs_.at[0], abr.at[0], sib)

    def start(h):
        for d in (1, 3, 2):
            send(spot(h, 0, 0), a1s.at[0], a1r.at[h, d - 1], peer(1 - h, d))

    def onward(h, s):
        if s:
            arrive(spot(h, 0, s), a1r.at[h, s - 1])
        for d in (2, 1, 3) if s == 2 else (1, 3):
            send(spot(h, 0, s), a2s.at[0], a2r.at[h, d - 1, s], peer(h, d))
        share(h, 0, s)

    relayed = {0: 1, 1: 3, 3: 1}

    def relay(h, s):
        for d in (1, 3):
            arrive(spot(h, d, s), a2r.at[h, d - 1, s])
            if relayed.get(s) == d:
                send(spot(h, d, s), a2s.at[0], a2r.at[h, 1, s], peer(h, d))
            share(h, d, s)

    def last(h, s):
        arrive(spot(h, 2, s), a2r.at[h, 1, s])
        share(h, 2, s)

    both(start)
    both(onward, 0)

    def rest_of_products():
        mom_o[...] = beta_first * state[0] + (1.0 - beta_first) * g_ref[...]
        q = parts(g_ref[...])
        ln_o[...] = beta_second * state[2] + (1.0 - beta_second) * mm3(q, q, 1, 1)
        qt = parts(g_ref[...].T)
        rn_o[...] = beta_second * state[3] + (1.0 - beta_second) * mm3(qt, q)

    def bases():
        lb_o[...] = wl[:, BLOCK:].T
        rb_o[...] = wr[:, BLOCK:].T

    work = [functools.partial(factor_block, k, wl, wr) for k in range(EARLY, BLOCK // NB)]
    work = work + [rest_of_products, bases]
    polls = {
        1: ((onward, 1), (onward, 3)),
        2: ((relay, 0), (onward, 2)),
        3: ((relay, 1),),
        4: ((last, 0), (relay, 3)),
        5: ((last, 1), (relay, 2)),
        len(work) - 1: ((last, 3), (last, 2)),
    }
    for i, do in enumerate(work):
        do()
        for q in polls.get(i, ()):
            both(*q)

    bytes_of(upd.at[0:2], abr.at[0])
    for ref, sem in ((f1, f1s), (msib, mss), (s2, s2s), (r1, s1s), (rsib, sbs), (f3, f3s)):
        bytes_of(ref, sem.at[0])
    bytes_of(r2, s3s.at[0])
    bytes_of(nrecv.at[0:others, :], nps.at[0])
    bytes_of(upd.at[0, 0:192, 0:1024], a1s.at[0])
    bytes_of(upd.at[0:3, 0:128, :], a2s.at[0])
    bytes_of(upd.at[0:2], abs_.at[0])


def store_kernel(*refs):
    m = len(refs) // 2
    sem = refs[-1]
    copies = [pltpu.make_async_copy(refs[i], refs[m + i], sem.at[i]) for i in range(m)]
    for q in copies:
        q.start()
    for q in copies:
        q.wait()


def on_device(nx, nz, ny, partials, *states):
    f32, bf16 = jnp.float32, jnp.bfloat16
    rows, width = partials.shape[1:]
    part = partials.reshape(nx, BLOCK, width)
    hbm = pl.BlockSpec(memory_space=pltpu.HBM)
    vmem = pl.BlockSpec(memory_space=pltpu.VMEM)
    ring = max(nx, nz)
    square = (BLOCK, BLOCK)
    dma = pltpu.SemaphoreType.DMA
    members = 2 * nx * nz
    shapes = [jax.ShapeDtypeStruct((nx, BLOCK, width), bf16)] + [jax.ShapeDtypeStruct(square, f32)] * 6
    outs = pl.pallas_call(
        functools.partial(kernel, nx, nz, ny),
        out_shape=shapes,
        in_specs=[hbm] * 7,
        out_specs=[vmem] * 7,
        scratch_shapes=[
            pltpu.VMEM((6, *square), f32),
            pltpu.VMEM((2, ring, BLOCK, 2 * BLOCK), bf16),
            pltpu.VMEM((2, ring, 2, QUART, 2 * BLOCK), bf16),
            pltpu.VMEM((2, ring, 2, 2, QUART, BLOCK), f32),
            pltpu.VMEM((2, ring, 2, QUART, BLOCK), f32),
            pltpu.VMEM((2, ring, 2, QUART, BLOCK), f32),
            pltpu.VMEM((2, ring, 2, QUART, 2 * BLOCK), bf16),
            pltpu.VMEM((2, 2, ring, 2, QUART, BLOCK), f32),
            pltpu.VMEM((2, ring, 2, QUART, BLOCK), f32),
            pltpu.VMEM((2, 2, QUART, BLOCK), f32),
            pltpu.VMEM((2, 2, 2, QUART, BLOCK), f32),
            pltpu.VMEM(square, f32),
            pltpu.VMEM((5, *square), f32),
            pltpu.VMEM((BLOCK, 2 * BLOCK), f32),
            pltpu.VMEM((BLOCK, 2 * BLOCK), f32),
            pltpu.VMEM((1, 128), f32),
            pltpu.VMEM((members * ny, 128), f32),
            dma((6,)), dma((2, ring)),
            dma((1,)), dma((2, ring)),
            dma((1,)), dma((2, ring)),
            dma((1,)), dma((2, ring)),
            dma((1,)), dma((2, ring)),
            dma((1,)), dma((2, ring)),
            dma((1,)), dma((2, 2)),
            dma((1,)), dma((2,)),
            dma((1,)), dma((1,)),
            dma((1,)), dma((2, ring - 1)),
            dma((1,)), dma((2, ring - 1, ring)),
            dma((1,)), dma((1,)),
        ],
        compiler_params=pltpu.CompilerParams(
            collective_id=0, has_side_effects=True, vmem_limit_bytes=36 * 1024 * 1024
        ),
    )(*(pltpu.with_memory_space_constraint(a, pltpu.HBM) for a in (part, *(s[0] for s in states))))
    outs = pl.pallas_call(
        store_kernel,
        out_shape=shapes,
        in_specs=[vmem] * 7,
        out_specs=[hbm] * 7,
        scratch_shapes=[dma((7,))],
        compiler_params=pltpu.CompilerParams(vmem_limit_bytes=8 * 1024 * 1024),
    )(*outs)
    return (outs[0].reshape(rows, width), *(o[None] for o in outs[1:]))


def solution(mesh):
    nx = nz = 4
    ny = mesh.shape["mp"]
    split = Mesh(mesh.devices.reshape(nx, nz, 2, ny), ("x", "z", "c", "y"))
    dp = ("x", "z", "c")
    whole = P(dp + ("y",), None, None)
    return jax.shard_map(
        functools.partial(on_device, nx, nz, ny),
        mesh=split,
        in_specs=(P(dp, None, "y"),) + (whole,) * 6,
        out_specs=(P(None, "y"),) + (whole,) * 6,
        check_vma=False,
    )
```
